256 devices in a mesh: row: 32 (over x, z_lo, core), chan: 8 (over y, z_hi).
Axes of the slice: x: 4, y: 4, z: 8 (z_hi: 2, z_lo: 4; z = z_hi * 4 + z_lo), core: 2. Of those that a mesh axis runs over, the one named last changes fastest.
Arguments:
- pair: bfloat16 [128, 768, 768], P('chan', 'row'), may hold values from -24 to 24
- single: bfloat16 [768, 384], P('row'), may hold values from -6 to 6
- token_mask: int32 [768], replicated, may hold values from 0 to 1, as said below
- pair_gain: float32 [128], replicated, may hold values from 0.5 to 1.5
- w_ab: bfloat16 [128, 4, 128], replicated, may hold values from -0.5 to 0.5
- w_out_gate: bfloat16 [128, 128], replicated, may hold values from -0.5 to 0.5
- x_gain: float32 [128], replicated, may hold values from 0.5 to 1.5
- w_tri_out: bfloat16 [128, 128], replicated, may hold values from -0.5 to 0.5
- bias_gain: float32 [128], replicated, may hold values from 0.5 to 1.5
- w_bias: bfloat16 [128, 16], replicated, may hold values from -0.5 to 0.5
- single_gain: float32 [384], replicated, may hold values from 0.5 to 1.5
- w_query: bfloat16 [384, 384], P(None, 'chan'), may hold values from -1 to 1
- w_key: bfloat16 [384, 384], P(None, 'chan'), may hold values from -16 to 16
- w_value_gate: bfloat16 [384, 2, 384], P(None, None, 'chan'), may hold values from -0.3125 to 0.3125
- w_mix: bfloat16 [384, 384], P('chan'), may hold values from -0.3125 to 0.3125
Outputs:
- pair_out: bfloat16 [128, 768, 768], P('chan', 'row')
- attended: bfloat16 [768, 384], P('row', 'chan')
The draws below stay inside these ranges and needn't reach their ends.
Inputs may be any that keep to these rules, and one draw needn't show every extreme that they name: token_mask is 1 on the first tokens and 0 on the rest; at least 672 tokens are real.
All inputs are finite; a program needn't handle non-finite values.
Results may differ from the reference program's by a relative error of at most 0.015.
The reference program's roundings to bfloat16 on the way count: a program that leaves them out, or rounds other values in their place, can miss the bound.
Values may be sent and summed in bfloat16 or wider, within the bound.
No kernel may reach another device: no remote copies, remote signals or barrier semaphores. Data moves between devices by JAX's collectives and lax.ppermute only.
A program may use at most 64 MiB of HBM per device.

```python
import math
import jax
import jax.numpy as jnp
from jax import lax

C = 128
D = 384
H = 16
N = 768


def shared_query(key):
    return jax.random.normal(jax.random.fold_in(key, 7), (D, D), jnp.float32) / math.sqrt(D)


def draw_pair(key, part):
    rough = jax.random.normal(key, (C, N, N), jnp.float32)
    return jnp.clip(rough, -6.0, 6.0).astype(jnp.bfloat16)


def draw_token_mask(key, part):
    picks = jax.random.randint(key, (N,), 0, 1 << 20, jnp.int32)
    length = N - N // 8 + picks[0] % (N // 8 + 1)
    positions = jnp.arange(N, dtype=jnp.int32)
    return (positions < length.astype(jnp.int32)).astype(jnp.int32)


def draw_w_query(key, part):
    return jnp.clip(shared_query(key), -1.0, 1.0).astype(jnp.bfloat16)


def draw_w_key(key, part):
    own = jax.random.normal(jax.random.fold_in(key, 8), (D, D), jnp.float32) / math.sqrt(D)
    return jnp.clip(own, -1.0, 1.0).astype(jnp.bfloat16)


def level_of(rng, shape, cuts, smallest, top_value):
    def one(dim, parts):
        steps = jax.random.uniform(jax.random.fold_in(jax.random.fold_in(rng, 6), dim), (parts,), jnp.float32, smallest / len(cuts), top_value / len(cuts))
        return jnp.repeat(jnp.exp(steps), shape[dim] // parts).reshape((-1,) + (1,) * (len(shape) - dim - 1))

    factor_of = one(*cuts[0])
    for cut in cuts[1:]:
        factor_of = factor_of * one(*cut)
    return factor_of


def gaussian(own_key, shape, scale, most, cuts=(), held_as=jnp.bfloat16):
    result = scale * jax.random.normal(own_key, shape, jnp.float32)
    if cuts:
        result = result * level_of(own_key, shape, cuts, -0.22, 0.18)
    return jnp.clip(result, -most, most).astype(held_as)


def setup_inputs(seed: int = 0) -> dict:
    key_list = jax.random.split(jax.random.key(seed), 16)
    return {
        "pair": draw_pair(jax.random.fold_in(key_list[15], 71), 0),
        "single": gaussian(key_list[1], (N, D), 1.0, 6.0, ((0, 32),)),
        "token_mask": draw_token_mask(jax.random.fold_in(key_list[15], 71), 0),
        "pair_gain": jnp.clip(1.0 + 0.1 * jax.random.normal(key_list[3], (C,), jnp.float32), 0.5, 1.5),
        "w_ab": gaussian(key_list[4], (C, 4, C), C ** -0.5, 0.5),
        "w_out_gate": gaussian(key_list[5], (C, C), C ** -0.5, 0.5),
        "x_gain": jnp.clip(1.0 + 0.1 * jax.random.normal(key_list[6], (C,), jnp.float32), 0.5, 1.5),
        "w_tri_out": gaussian(key_list[7], (C, C), C ** -0.5, 0.5),
        "bias_gain": jnp.clip(1.0 + 0.1 * jax.random.normal(key_list[8], (C,), jnp.float32), 0.5, 1.5),
        "w_bias": gaussian(key_list[9], (C, H), C ** -0.5, 0.5),
        "single_gain": jnp.clip(1.0 + 0.1 * jax.random.normal(key_list[10], (D,), jnp.float32), 0.5, 1.5),
        "w_query": draw_w_query(jax.random.fold_in(key_list[15], 71), 0),
        "w_key": draw_w_key(jax.random.fold_in(key_list[15], 71), 0),
        "w_value_gate": gaussian(key_list[13], (D, 2, D), D ** -0.5, 0.3125, ((2, 8),)),
        "w_mix": gaussian(key_list[14], (D, D), D ** -0.5, 0.3125, ((0, 8),)),
    }


EPS = 1e-05

def layer_norm(values, gain, axis):
    middle = lax.optimization_barrier(jnp.mean(values, axis=axis, keepdims=True))
    centred = values - middle
    spread = lax.optimization_barrier(jnp.mean(centred * centred, axis=axis, keepdims=True))
    return centred * lax.rsqrt(spread + EPS) * gain

def project(normed, weight):
    return jnp.einsum('cij,cd->dij', normed.astype(jnp.float32), weight.astype(jnp.float32))

def edge(normed, w_gate, w_value, pair_mask):
    opened = jax.nn.sigmoid(project(normed, w_gate))
    return (opened * project(normed, w_value) * pair_mask[None]).astype(jnp.bfloat16)

def reference(pair, single, token_mask, pair_gain, w_ab, w_out_gate, x_gain, w_tri_out, bias_gain, w_bias, single_gain, w_query, w_key, w_value_gate, w_mix):
    live = token_mask.astype(jnp.float32)
    pair_mask = live[:, None] * live[None, :]
    wide = pair.astype(jnp.float32)
    normed = layer_norm(wide, pair_gain[:, None, None], 0).astype(jnp.bfloat16)
    left = edge(normed, w_ab[:, 0], w_ab[:, 1], pair_mask)
    right = edge(normed, w_ab[:, 2], w_ab[:, 3], pair_mask)
    product = jnp.einsum('cik,cjk->cij', left.astype(jnp.float32), right.astype(jnp.float32)).astype(jnp.bfloat16)
    product_normed = layer_norm(product.astype(jnp.float32), x_gain[:, None, None], 0).astype(jnp.bfloat16)
    out_gate = jax.nn.sigmoid(project(normed, w_out_gate))
    pair_out = (wide + out_gate * project(product_normed, w_tri_out)).astype(jnp.bfloat16)
    bias_input = layer_norm(pair_out.astype(jnp.float32), bias_gain[:, None, None], 0).astype(jnp.bfloat16)
    bias = jnp.einsum('cij,ch->hij', bias_input.astype(jnp.float32), w_bias.astype(jnp.float32))
    head_size = D // H
    single_normed = layer_norm(single.astype(jnp.float32), single_gain[None, :], 1).astype(jnp.bfloat16)
    queries = jnp.dot(single_normed, w_query, preferred_element_type=jnp.float32).astype(jnp.bfloat16)
    keys = jnp.dot(single_normed, w_key, preferred_element_type=jnp.float32).astype(jnp.bfloat16)
    values = jnp.dot(single_normed, w_value_gate[:, 0, :], preferred_element_type=jnp.float32).astype(jnp.bfloat16)
    head_gate = jax.nn.sigmoid(jnp.dot(single_normed, w_value_gate[:, 1, :], preferred_element_type=jnp.float32))
    query_heads = queries.astype(jnp.float32).reshape(N, H, head_size)
    key_heads = keys.astype(jnp.float32).reshape(N, H, head_size)
    value_heads = values.astype(jnp.float32).reshape(N, H, head_size)
    scores = jnp.einsum('ihe,jhe->hij', query_heads, key_heads) / jnp.sqrt(jnp.float32(head_size)) + bias
    scores = jnp.where(live[None, None, :] > 0, scores, -jnp.inf)
    top = lax.optimization_barrier(jnp.max(scores, axis=2, keepdims=True))
    raised = jnp.exp(scores - top)
    weights = (raised / lax.optimization_barrier(jnp.sum(raised, axis=2, keepdims=True))).astype(jnp.bfloat16)
    mixed = jnp.einsum('hij,jhe->ihe', weights.astype(jnp.float32), value_heads).reshape(N, D)
    heads_out = (mixed * head_gate).astype(jnp.bfloat16)
    attended = jnp.dot(heads_out, w_mix, preferred_element_type=jnp.float32).astype(jnp.bfloat16)
    return (pair_out, attended)
```

```python
import jax
import jax.numpy as jnp
from jax import lax
from jax.sharding import Mesh
from jax.sharding import PartitionSpec as P

D = 384
H = 16
C = 128
EPS = 1e-05
ROW = ("x", "zl", "core")
CHAN = ("y", "zh")
OWN = ("x", "zl", "y", "zh")
BF = jnp.bfloat16
F32 = jnp.float32


def layer_norm(values, gain, axis):
    middle = jnp.mean(values, axis=axis, keepdims=True)
    centred = values - middle
    spread = jnp.mean(centred * centred, axis=axis, keepdims=True)
    return centred * lax.rsqrt(spread + EPS) * gain


def swap(shard, axes):
    return lax.all_to_all(shard, axes, 0, 0, tiled=True)


def body(
    pair,
    single,
    token_mask,
    pair_gain,
    w_ab,
    w_out_gate,
    x_gain,
    w_tri_out,
    bias_gain,
    w_bias,
    single_gain,
    w_query,
    w_key,
    w_value_gate,
    w_mix,
):
    chans, rows, width = pair.shape
    nq = C // chans
    nrow = lax.axis_size(ROW)
    part = rows // nq
    spots = part * width
    r = lax.axis_index(ROW)
    q = lax.axis_index(CHAN)
    core = lax.axis_index("core")
    live = token_mask.astype(F32)

    single_normed = layer_norm(single.astype(F32), single_gain[None, :], 1).astype(BF)
    own_keys = jnp.dot(single_normed, w_key, preferred_element_type=F32).astype(BF)
    own_values = jnp.dot(single_normed, w_value_gate[:, 0, :], preferred_element_type=F32).astype(BF)
    own_kv = jnp.concatenate([own_keys, own_values], axis=1)
    kv = swap(jnp.broadcast_to(own_kv[None], (nrow,) + own_kv.shape), ROW)
    queries = jnp.dot(single_normed, w_query, preferred_element_type=F32).astype(BF)
    head_gate = jax.nn.sigmoid(
        jnp.dot(single_normed, w_value_gate[:, 1, :], preferred_element_type=F32)
    )

    sent = pair.reshape(chans, nq, spots).transpose(1, 0, 2)
    full = swap(sent, CHAN).reshape(C, spots).astype(F32)
    normed = layer_norm(full, pair_gain[:, None], 0).astype(BF)
    live_rows = lax.dynamic_slice_in_dim(live, r * rows + q * part, part, 0)
    mask = (live_rows[:, None] * live[None, :]).reshape(1, spots)
    projected = jnp.einsum("cp,ckd->kdp", normed, w_ab, preferred_element_type=F32)
    left = (jax.nn.sigmoid(projected[0]) * projected[1] * mask).astype(BF)
    right = (jax.nn.sigmoid(projected[2]) * projected[3] * mask).astype(BF)

    edges = swap(jnp.stack([left, right], axis=1), OWN)
    left_owned = edges[:, 0].reshape(C * part, width)
    right_here = edges[:, 1].reshape(C // nq, rows, width)
    right_there = lax.ppermute(right_here, "core", [(0, 1), (1, 0)])
    first = core == 0
    right_owned = jnp.stack(
        [
            jnp.where(first, right_here, right_there),
            jnp.where(first, right_there, right_here),
        ],
        axis=1,
    ).reshape(2 * C * part, width)
    owned = lax.dot_general(
        left_owned, right_owned, (((1,), (1,)), ((), ())), preferred_element_type=F32
    ).astype(BF)
    product = swap(owned.reshape(C, part, width), OWN).reshape(C, spots)

    product_normed = layer_norm(product.astype(F32), x_gain[:, None], 0).astype(BF)
    out_gate = jax.nn.sigmoid(
        jnp.einsum("cp,cd->dp", normed, w_out_gate, preferred_element_type=F32)
    )
    update = jnp.einsum("cp,cd->dp", product_normed, w_tri_out, preferred_element_type=F32)
    renewed = (full + out_gate * update).astype(BF)
    bias_input = layer_norm(renewed.astype(F32), bias_gain[:, None], 0).astype(BF)
    bias = jnp.einsum("cp,ch->hp", bias_input, w_bias, preferred_element_type=F32)

    head_size = D // H
    local_width = w_query.shape[1]
    heads = local_width // head_size
    bias = swap(bias.reshape(nq, heads, spots), CHAN)
    bias = bias.transpose(1, 0, 2).reshape(heads, rows, width)
    pair_out = swap(renewed.reshape(nq, chans, spots), CHAN)
    pair_out = pair_out.transpose(1, 0, 2).reshape(chans, rows, width)

    keys = kv[..., :local_width].reshape(-1, heads, head_size)
    values = kv[..., local_width:].reshape(-1, heads, head_size)
    query_heads = queries.reshape(rows, heads, head_size)
    scores = jnp.einsum("ihe,jhe->hij", query_heads, keys, preferred_element_type=F32)
    scores = scores / jnp.sqrt(F32(head_size)) + bias
    scores = jnp.where(live[None, None, :] > 0, scores, -jnp.inf)
    top = jnp.max(scores, axis=2, keepdims=True)
    raised = jnp.exp(scores - top)
    weights = (raised / jnp.sum(raised, axis=2, keepdims=True)).astype(BF)
    mixed = jnp.einsum("hij,jhe->ihe", weights, values, preferred_element_type=F32)
    heads_out = (mixed.reshape(rows, local_width) * head_gate).astype(BF)
    terms = jnp.dot(heads_out, w_mix, preferred_element_type=F32).astype(BF)
    terms = swap(terms.reshape(rows, nq, -1).transpose(1, 0, 2), CHAN)
    attended = jnp.sum(terms.astype(F32), axis=0).astype(BF)
    return (pair_out, attended)


def solution(mesh):
    split = Mesh(mesh.devices.reshape(4, 4, 2, 4, 2), ROW + CHAN)
    return jax.shard_map(
        body,
        mesh=split,
        in_specs=(
            P(CHAN, ROW, None),
            P(ROW, None),
            P(),
            P(),
            P(),
            P(),
            P(),
            P(),
            P(),
            P(),
            P(),
            P(None, CHAN),
            P(None, CHAN),
            P(None, None, CHAN),
            P(CHAN, None),
        ),
        out_specs=(P(CHAN, ROW, None), P(ROW, CHAN)),
        check_vma=False,
    )
```

```python
import jax
import jax.numpy as jnp
from jax import lax
from jax.sharding import Mesh
from jax.sharding import PartitionSpec as P

D = 384
H = 16
C = 128
EPS = 1e-05
ROW = ("x", "zl", "core")
CHAN = ("y", "zh")
OWN = ("x", "zl", "y", "zh")
BF = jnp.bfloat16
F32 = jnp.float32


def layer_norm(values, gain, axis):
    middle = jnp.mean(values, axis=axis, keepdims=True)
    centred = values - middle
    spread = jnp.mean(centred * centred, axis=axis, keepdims=True)
    return centred * lax.rsqrt(spread + EPS) * gain


def swap(shard, axes):
    return lax.all_to_all(shard, axes, 0, 0, tiled=True)


def doubled(block, axis, bit):
    size = lax.axis_size(axis)
    there = lax.ppermute(block, axis, [(i, i ^ (1 << bit)) for i in range(size)])
    low = (lax.axis_index(axis) >> bit) & 1 == 0
    return jnp.concatenate([jnp.where(low, block, there), jnp.where(low, there, block)], axis=0)


def edge(normed, w_gate, w_value, mask):
    opened = jnp.einsum("cp,cd->dp", normed, w_gate, preferred_element_type=F32)
    value = jnp.einsum("cp,cd->dp", normed, w_value, preferred_element_type=F32)
    return (jax.nn.sigmoid(opened) * value * mask).astype(BF)


def block(
    pair,
    single,
    token_mask,
    pair_gain,
    w_ab,
    w_out_gate,
    x_gain,
    w_tri_out,
    bias_gain,
    w_bias,
    single_gain,
    w_query,
    w_key,
    w_value_gate,
    w_mix,
):
    chans, rows, width = pair.shape
    nq = C // chans
    part = rows // nq
    spots = part * width
    r = lax.axis_index(ROW)
    q = lax.axis_index(CHAN)
    core = lax.axis_index("core")
    live = token_mask.astype(F32)

    single_normed = layer_norm(single.astype(F32), single_gain[None, :], 1).astype(BF)
    own_keys = jnp.dot(single_normed, w_key, preferred_element_type=F32).astype(BF)
    own_values = jnp.dot(single_normed, w_value_gate[:, 0, :], preferred_element_type=F32).astype(BF)
    own_kv = jnp.concatenate([own_keys, own_values], axis=1)
    kv = own_kv
    for axis, bit in (("core", 0), ("zl", 0), ("zl", 1), ("x", 0)):
        kv = doubled(kv, axis, bit)
    queries = jnp.dot(single_normed, w_query, preferred_element_type=F32).astype(BF)
    head_gate = jax.nn.sigmoid(
        jnp.dot(single_normed, w_value_gate[:, 1, :], preferred_element_type=F32)
    )

    sent = pair.reshape(chans, nq, spots).transpose(1, 0, 2)
    full = swap(sent, CHAN).reshape(C, spots).astype(F32)
    normed = layer_norm(full, pair_gain[:, None], 0).astype(BF)
    live_rows = lax.dynamic_slice_in_dim(live, r * rows + q * part, part, 0)
    mask = (live_rows[:, None] * live[None, :]).reshape(1, spots)
    left = edge(normed, w_ab[:, 0], w_ab[:, 1], mask).reshape(C, 2, spots // 2)
    right = edge(normed, w_ab[:, 2], w_ab[:, 3], mask).reshape(C, 2, spots // 2)
    edges = swap(jnp.concatenate([right, left], axis=2), OWN)
    right_here = edges[:, :, : spots // 2].reshape(C // nq, rows, width)
    right_there = lax.ppermute(right_here, "core", [(0, 1), (1, 0)])
    left_owned = edges[:, :, spots // 2 :].reshape(C * part, width)
    left_owned, kv = lax.optimization_barrier((left_owned, kv))
    kv = doubled(kv, "x", 1)
    first = core == 0
    right_owned = jnp.stack(
        [
            jnp.where(first, right_here, right_there),
            jnp.where(first, right_there, right_here),
        ],
        axis=1,
    ).reshape(2 * C * part, width)
    owned = lax.dot_general(
        left_owned, right_owned, (((1,), (1,)), ((), ())), preferred_element_type=F32
    ).astype(BF)
    product = swap(owned.reshape(C, 2, spots // 2), OWN).reshape(C, spots)
    product, kv = lax.optimization_barrier((product, kv))

    product_normed = layer_norm(product.astype(F32), x_gain[:, None], 0).astype(BF)
    out_gate = jax.nn.sigmoid(
        jnp.einsum("cp,cd->dp", normed, w_out_gate, preferred_element_type=F32)
    )
    update = jnp.einsum("cp,cd->dp", product_normed, w_tri_out, preferred_element_type=F32)
    renewed = (full + out_gate * update).astype(BF)
    bias_input = layer_norm(renewed.astype(F32), bias_gain[:, None], 0).astype(BF)
    bias = jnp.einsum("cp,ch->hp", bias_input, w_bias, preferred_element_type=F32)

    head_size = D // H
    local_width = w_query.shape[1]
    heads = local_width // head_size
    bias = swap(bias.reshape(nq, heads, spots), CHAN)
    bias = bias.transpose(1, 0, 2).reshape(heads, rows, width)
    keys = kv[:, :local_width].reshape(-1, heads, head_size)
    values = kv[:, local_width:].reshape(-1, heads, head_size)
    query_heads = queries.reshape(rows, heads, head_size)
    scores = jnp.einsum("ihe,jhe->hij", query_heads, keys, preferred_element_type=F32)
    scores = scores / jnp.sqrt(F32(head_size)) + bias
    scores = jnp.where(live[None, None, :] > 0, scores, -jnp.inf)
    top = jnp.max(scores, axis=2, keepdims=True)
    raised = jnp.exp(scores - top)
    weights = (raised / jnp.sum(raised, axis=2, keepdims=True)).astype(BF)
    mixed = jnp.einsum("hij,jhe->ihe", weights, values, preferred_element_type=F32)
    heads_out = (mixed.reshape(rows, local_width) * head_gate).astype(BF)
    terms = jnp.dot(heads_out, w_mix, preferred_element_type=F32).astype(BF)
    terms = terms.reshape(rows, nq, local_width).transpose(1, 0, 2).reshape(nq, -1, 128)
    terms = jnp.pad(terms, ((0, 0), (0, chans - terms.shape[1]), (0, 0)))
    sent = jnp.concatenate([renewed.reshape(nq, chans, spots), terms], axis=2)
    both = swap(sent, CHAN)
    pair_out = both[:, :, :spots].transpose(1, 0, 2).reshape(chans, rows, width)
    terms = both[:, : rows * local_width // 128, spots:].reshape(nq, rows, local_width)
    attended = jnp.sum(terms.astype(F32), axis=0).astype(BF)
    return (pair_out, attended)


def solution(mesh):
    split = Mesh(mesh.devices.reshape(4, 4, 2, 4, 2), ROW + CHAN)
    return jax.shard_map(
        block,
        mesh=split,
        in_specs=(
            P(CHAN, ROW, None),
            P(ROW, None),
            P(),
            P(),
            P(),
            P(),
            P(),
            P(),
            P(),
            P(),
            P(),
            P(None, CHAN),
            P(None, CHAN),
            P(None, None, CHAN),
            P(CHAN, None),
        ),
        out_specs=(P(CHAN, ROW, None), P(ROW, CHAN)),
        check_vma=False,
    )
```

```python
import jax
import jax.numpy as jnp
from jax import lax
from jax.sharding import Mesh
from jax.sharding import PartitionSpec as P

D = 384
H = 16
C = 128
EPS = 1e-05
LANES = 128
ROW = ("x", "zl", "core")
CHAN = ("y", "zh")
OWN = ("x", "zl", "y", "zh")
BF = jnp.bfloat16
F32 = jnp.float32


def layer_norm(values, gain, axis):
    middle = jnp.mean(values, axis=axis, keepdims=True)
    centred = values - middle
    spread = jnp.mean(centred * centred, axis=axis, keepdims=True)
    return centred * lax.rsqrt(spread + EPS) * gain


def swap(shard, axes):
    return lax.all_to_all(shard, axes, 0, 0, tiled=True)


def doubled(block, axis, bit, dim):
    size = lax.axis_size(axis)
    there = lax.ppermute(block, axis, [(i, i ^ (1 << bit)) for i in range(size)])
    low = (lax.axis_index(axis) >> bit) & 1 == 0
    return jnp.concatenate([jnp.where(low, block, there), jnp.where(low, there, block)], axis=dim)


def filled(*parts):
    wide = jnp.concatenate(parts, axis=1)
    return jnp.pad(wide, ((0, 0), (0, LANES - wide.shape[1])))


def edge(normed, w_gate, w_value, mask):
    opened = jnp.einsum("cp,cd->dp", normed, w_gate, preferred_element_type=F32)
    value = jnp.einsum("cp,cd->dp", normed, w_value, preferred_element_type=F32)
    return (jax.nn.sigmoid(opened) * value * mask).astype(BF)


def block(
    pair,
    single,
    token_mask,
    pair_gain,
    w_ab,
    w_out_gate,
    x_gain,
    w_tri_out,
    bias_gain,
    w_bias,
    single_gain,
    w_query,
    w_key,
    w_value_gate,
    w_mix,
):
    chans, rows, width = pair.shape
    nq = C // chans
    part = rows // nq
    spots = part * width
    r = lax.axis_index(ROW)
    q = lax.axis_index(CHAN)
    core = lax.axis_index("core")
    live = token_mask.astype(F32)

    single_normed = layer_norm(single.astype(F32), single_gain[None, :], 1).astype(BF)
    own_keys = jnp.dot(single_normed, w_key, preferred_element_type=F32).astype(BF)
    own_values = jnp.dot(single_normed, w_value_gate[:, 0, :], preferred_element_type=F32).astype(BF)
    queries = jnp.dot(single_normed, w_query, preferred_element_type=F32).astype(BF)
    head_gate = jax.nn.sigmoid(
        jnp.dot(single_normed, w_value_gate[:, 1, :], preferred_element_type=F32)
    )
    gate_high = lax.reduce_precision(head_gate, 8, 7)
    gate_rest = (head_gate - gate_high).astype(BF)
    local = w_query.shape[1]
    kv = filled(own_keys, own_values)
    rest = jnp.concatenate(
        [filled(queries, gate_high.astype(BF)), filled(gate_rest)]
        + [w_mix[:, k : k + LANES] for k in range(0, D, LANES)]
    )
    both = doubled(jnp.concatenate([kv, rest])[None], "zh", 0, 0)
    kv, rest = both[:, :rows], both[:, rows:]
    kv = doubled(kv, "zl", 0, 1)
    kv = doubled(kv, "zl", 1, 1)
    both = jnp.concatenate([kv, rest], axis=1)
    both = doubled(both, "y", 0, 0)
    both = doubled(both, "y", 1, 0)
    kv, rest = both[:, : kv.shape[1]], both[:, kv.shape[1] :]
    kv = doubled(kv[:, None, None], "x", 1, 1)
    kv = doubled(kv, "x", 0, 2)
    kv = doubled(kv.reshape(nq, -1, 1, rows, LANES), "core", 0, 2)
    kv = kv.reshape(nq, -1, LANES)

    sent = pair.reshape(chans, nq, spots).transpose(1, 0, 2)
    full = swap(sent, CHAN).reshape(C, spots).astype(F32)
    normed = layer_norm(full, pair_gain[:, None], 0).astype(BF)
    live_rows = lax.dynamic_slice_in_dim(live, r * rows + q * part, part, 0)
    mask = (live_rows[:, None] * live[None, :]).reshape(1, spots)
    left = edge(normed, w_ab[:, 0], w_ab[:, 1], mask).reshape(C, 2, spots // 2)
    right = edge(normed, w_ab[:, 2], w_ab[:, 3], mask).reshape(C, 2, spots // 2)
    edges = swap(jnp.concatenate([right, left], axis=2), OWN)
    right_here = edges[:, :, : spots // 2].reshape(C // nq, rows, width)
    right_there = lax.ppermute(right_here, "core", [(0, 1), (1, 0)])
    left_owned = edges[:, :, spots // 2 :].reshape(C * part, width)
    first = core == 0
    right_owned = jnp.stack(
        [
            jnp.where(first, right_here, right_there),
            jnp.where(first, right_there, right_here),
        ],
        axis=1,
    ).reshape(2 * C * part, width)
    owned = lax.dot_general(
        left_owned, right_owned, (((1,), (1,)), ((), ())), preferred_element_type=F32
    ).astype(BF)
    product = swap(owned.reshape(C, 2, spots // 2), OWN).reshape(C, spots)

    product_normed = layer_norm(product.astype(F32), x_gain[:, None], 0).astype(BF)
    out_gate = jax.nn.sigmoid(
        jnp.einsum("cp,cd->dp", normed, w_out_gate, preferred_element_type=F32)
    )
    update = jnp.einsum("cp,cd->dp", product_normed, w_tri_out, preferred_element_type=F32)
    renewed = (full + out_gate * update).astype(BF)
    bias_input = layer_norm(renewed.astype(F32), bias_gain[:, None], 0).astype(BF)
    bias = jnp.einsum("cp,ch->hp", bias_input, w_bias, preferred_element_type=F32)

    heads = H // nq
    head_size = D // H
    at = q * part
    mine = lax.dynamic_slice_in_dim(rest, at, part, 1)
    gate_mine = mine[..., local : 2 * local].astype(F32) + lax.dynamic_slice_in_dim(
        rest, rows + at, part, 1
    )[..., :local].astype(F32)
    is_head = (jnp.arange(local)[None, :] // head_size == jnp.arange(heads)[:, None])[:, None]
    queries = jnp.where(is_head, mine[:, None, :, :local], 0).reshape(nq, heads * part, local)
    scores = jnp.einsum("qaf,qjf->qaj", queries, kv[..., :local], preferred_element_type=F32)
    scores = scores / jnp.sqrt(F32(head_size)) + bias.reshape(nq, heads * part, width)
    scores = jnp.where(live[None, None, :] > 0, scores, -jnp.inf)
    top = jnp.max(scores, axis=2, keepdims=True)
    raised = jnp.exp(scores - top)
    weights = (raised / jnp.sum(raised, axis=2, keepdims=True)).astype(BF)
    mixed = jnp.einsum(
        "qaj,qjf->qaf", weights, kv[..., local : 2 * local], preferred_element_type=F32
    )
    mixed = jnp.where(is_head, mixed.reshape(nq, heads, part, local), 0).sum(axis=1)
    heads_out = (mixed * gate_mine).astype(BF).transpose(1, 0, 2).reshape(part, D)
    mix = rest[:, 2 * rows :].reshape(nq, D // LANES, local, LANES).transpose(0, 2, 1, 3)
    summed = jnp.dot(heads_out, mix.reshape(D, D), preferred_element_type=F32).astype(BF)
    summed = summed.reshape(part, nq, local).transpose(1, 0, 2)
    summed = jnp.pad(summed, ((0, 0), (0, chans - part), (0, LANES - local)))
    sent = jnp.concatenate([renewed.reshape(nq, chans, spots), summed], axis=2)
    both = swap(sent, CHAN)
    pair_out = both[:, :, :spots].transpose(1, 0, 2).reshape(chans, rows, width)
    attended = both[:, :part, spots : spots + local].reshape(rows, local)
    return (pair_out, attended)


def solution(mesh):
    split = Mesh(mesh.devices.reshape(4, 4, 2, 4, 2), ROW + CHAN)
    return jax.shard_map(
        block,
        mesh=split,
        in_specs=(
            P(CHAN, ROW, None),
            P(ROW, None),
            P(),
            P(),
            P(),
            P(),
            P(),
            P(),
            P(),
            P(),
            P(),
            P(None, CHAN),
            P(None, CHAN),
            P(None, None, CHAN),
            P(CHAN, None),
        ),
        out_specs=(P(CHAN, ROW, None), P(ROW, CHAN)),
        check_vma=False,
    )
```

```python
import jax
import jax.numpy as jnp
from jax import lax
from jax.sharding import Mesh
from jax.sharding import PartitionSpec as P

D = 384
H = 16
C = 128
EPS = 1e-05
LANES = 128
ROW = ("x", "zl", "core")
CHAN = ("y", "zh")
OWN = ("x", "zl", "y", "zh")
BF = jnp.bfloat16
F32 = jnp.float32


def layer_norm(values, gain, axis):
    middle = jnp.mean(values, axis=axis, keepdims=True)
    centred = values - middle
    spread = jnp.mean(centred * centred, axis=axis, keepdims=True)
    return centred * lax.rsqrt(spread + EPS) * gain


def swap(shard, axes):
    return lax.all_to_all(shard, axes, 0, 0, tiled=True)


def doubled(block, axis, bit, dim):
    size = lax.axis_size(axis)
    there = lax.ppermute(block, axis, [(i, i ^ (1 << bit)) for i in range(size)])
    low = (lax.axis_index(axis) >> bit) & 1 == 0
    return jnp.concatenate([jnp.where(low, block, there), jnp.where(low, there, block)], axis=dim)


def filled(*parts):
    wide = jnp.concatenate(parts, axis=-1)
    return jnp.pad(wide, [(0, 0)] * (wide.ndim - 1) + [(0, LANES - wide.shape[-1])])


def edge(normed, w_gate, w_value, mask):
    opened = jnp.einsum("cp,cd->dp", normed, w_gate, preferred_element_type=F32)
    value = jnp.einsum("cp,cd->dp", normed, w_value, preferred_element_type=F32)
    return (jax.nn.sigmoid(opened) * value * mask).astype(BF)


def block(
    pair,
    single,
    token_mask,
    pair_gain,
    w_ab,
    w_out_gate,
    x_gain,
    w_tri_out,
    bias_gain,
    w_bias,
    single_gain,
    w_query,
    w_key,
    w_value_gate,
    w_mix,
):
    chans, rows, width = pair.shape
    nq = C // chans
    part = rows // nq
    spots = part * width
    r = lax.axis_index(ROW)
    q = lax.axis_index(CHAN)
    core = lax.axis_index("core")
    live = token_mask.astype(F32)

    local = w_query.shape[1]
    weights = [w_query, w_key, w_value_gate[:, 0, :], w_value_gate[:, 1, :]]
    weights = jnp.concatenate([w.T for w in weights] + [w_mix], axis=0)
    weights = doubled(weights[None], "zh", 0, 0)
    single_normed = layer_norm(single.astype(F32), single_gain[None, :], 1).astype(BF)
    projected = jnp.einsum(
        "tf,zof->zto", single_normed, weights[:, : 4 * local], preferred_element_type=F32
    )
    head_gate = jax.nn.sigmoid(projected[..., 3 * local :])
    gate_high = lax.reduce_precision(head_gate, 8, 7)
    gate_rest = (head_gate - gate_high).astype(BF)
    kv = filled(projected[..., local : 3 * local].astype(BF))
    rest = jnp.concatenate(
        [
            filled(projected[..., :local].astype(BF), gate_high.astype(BF)),
            filled(gate_rest),
        ]
        + [weights[:, 4 * local :, k : k + LANES] for k in range(0, D, LANES)],
        axis=1,
    )
    kv = kv[None, None, :, None, None, None, None, None]
    kv = doubled(kv, "y", 1, 0)
    kv = doubled(kv, "x", 1, 3)
    kv = doubled(kv, "zl", 1, 5)
    kv = doubled(kv, "zl", 0, 6)
    kv = doubled(kv, "y", 0, 1)
    kv = doubled(kv, "x", 0, 4)
    kv = doubled(kv, "core", 0, 7)
    kv = kv.reshape(nq, -1, LANES)
    rest = doubled(rest, "y", 0, 0)
    rest = doubled(rest, "y", 1, 0)

    sent = pair.reshape(chans, nq, spots).transpose(1, 0, 2)
    full = swap(sent, CHAN).reshape(C, spots).astype(F32)
    normed = layer_norm(full, pair_gain[:, None], 0).astype(BF)
    live_rows = lax.dynamic_slice_in_dim(live, r * rows + q * part, part, 0)
    mask = (live_rows[:, None] * live[None, :]).reshape(1, spots)
    left = edge(normed, w_ab[:, 0], w_ab[:, 1], mask).reshape(C, 2, spots // 2)
    right = edge(normed, w_ab[:, 2], w_ab[:, 3], mask).reshape(C, 2, spots // 2)
    edges = swap(jnp.concatenate([right, left], axis=2), OWN)
    right_here = edges[:, :, : spots // 2].reshape(C // nq, rows, width)
    right_there = lax.ppermute(right_here, "core", [(0, 1), (1, 0)])
    left_owned = edges[:, :, spots // 2 :].reshape(C * part, width)
    first = core == 0
    right_owned = jnp.stack(
        [
            jnp.where(first, right_here, right_there),
            jnp.where(first, right_there, right_here),
        ],
        axis=1,
    ).reshape(2 * C * part, width)
    owned = lax.dot_general(
        left_owned, right_owned, (((1,), (1,)), ((), ())), preferred_element_type=F32
    ).astype(BF)
    product = swap(owned.reshape(C, 2, spots // 2), OWN).reshape(C, spots)

    product_normed = layer_norm(product.astype(F32), x_gain[:, None], 0).astype(BF)
    out_gate = jax.nn.sigmoid(
        jnp.einsum("cp,cd->dp", normed, w_out_gate, preferred_element_type=F32)
    )
    update = jnp.einsum("cp,cd->dp", product_normed, w_tri_out, preferred_element_type=F32)
    renewed = (full + out_gate * update).astype(BF)
    bias_input = layer_norm(renewed.astype(F32), bias_gain[:, None], 0).astype(BF)
    bias = jnp.einsum("cp,ch->hp", bias_input, w_bias, preferred_element_type=F32)

    heads = H // nq
    head_size = D // H
    at = q * part
    mine = lax.dynamic_slice_in_dim(rest, at, part, 1)
    gate_mine = mine[..., local : 2 * local].astype(F32) + lax.dynamic_slice_in_dim(
        rest, rows + at, part, 1
    )[..., :local].astype(F32)
    is_head = (jnp.arange(local)[None, :] // head_size == jnp.arange(heads)[:, None])[:, None]
    queries = jnp.where(is_head, mine[:, None, :, :local], 0).reshape(nq, heads * part, local)
    scores = jnp.einsum("qaf,qjf->qaj", queries, kv[..., :local], preferred_element_type=F32)
    scores = scores / jnp.sqrt(F32(head_size)) + bias.reshape(nq, heads * part, width)
    scores = jnp.where(live[None, None, :] > 0, scores, -jnp.inf)
    top = jnp.max(scores, axis=2, keepdims=True)
    raised = jnp.exp(scores - top)
    weights = (raised / jnp.sum(raised, axis=2, keepdims=True)).astype(BF)
    mixed = jnp.einsum(
        "qaj,qjf->qaf", weights, kv[..., local : 2 * local], preferred_element_type=F32
    )
    mixed = jnp.where(is_head, mixed.reshape(nq, heads, part, local), 0).sum(axis=1)
    heads_out = (mixed * gate_mine).astype(BF).transpose(1, 0, 2).reshape(part, D)
    mix = rest[:, 2 * rows :].reshape(nq, D // LANES, local, LANES).transpose(0, 2, 1, 3)
    summed = jnp.dot(heads_out, mix.reshape(D, D), preferred_element_type=F32).astype(BF)
    summed = summed.reshape(part, nq, local).transpose(1, 0, 2)
    summed = jnp.pad(summed, ((0, 0), (0, chans - part), (0, LANES - local)))
    sent = jnp.concatenate([renewed.reshape(nq, chans, spots), summed], axis=2)
    both = swap(sent, CHAN)
    pair_out = both[:, :, :spots].transpose(1, 0, 2).reshape(chans, rows, width)
    attended = both[:, :part, spots : spots + local].reshape(rows, local)
    return (pair_out, attended)


def solution(mesh):
    split = Mesh(mesh.devices.reshape(4, 4, 2, 4, 2), ROW + CHAN)
    return jax.shard_map(
        block,
        mesh=split,
        in_specs=(
            P(CHAN, ROW, None),
            P(ROW, None),
            P(),
            P(),
            P(),
            P(),
            P(),
            P(),
            P(),
            P(),
            P(),
            P(None, CHAN),
            P(None, CHAN),
            P(None, None, CHAN),
            P(CHAN, None),
        ),
        out_specs=(P(CHAN, ROW, None), P(ROW, CHAN)),
        check_vma=False,
    )
```

```python
import jax
import jax.numpy as jnp
from jax import lax
from jax.sharding import Mesh
from jax.sharding import PartitionSpec as P

D = 384
H = 16
C = 128
EPS = 1e-05
LANES = 128
ROW = ("x", "zl", "core")
CHAN = ("y", "zh")
OWN = ("x", "zl", "y", "zh")
BF = jnp.bfloat16
F32 = jnp.float32


def layer_norm(values, gain, axis):
    middle = jnp.mean(values, axis=axis, keepdims=True)
    centred = values - middle
    spread = jnp.mean(centred * centred, axis=axis, keepdims=True)
    return centred * lax.rsqrt(spread + EPS) * gain


def swap(shard, axes):
    return lax.all_to_all(shard, axes, 0, 0, tiled=True)


def doubled(block, axis, bit, dim):
    size = lax.axis_size(axis)
    there = lax.ppermute(block, axis, [(i, i ^ (1 << bit)) for i in range(size)])
    low = (lax.axis_index(axis) >> bit) & 1 == 0
    return jnp.concatenate([jnp.where(low, block, there), jnp.where(low, there, block)], axis=dim)


def filled(*parts):
    wide = jnp.concatenate(parts, axis=-1)
    return jnp.pad(wide, [(0, 0)] * (wide.ndim - 1) + [(0, LANES - wide.shape[-1])])


def edge(normed, w_gate, w_value, mask):
    opened = jnp.einsum("cp,cd->dp", normed, w_gate, preferred_element_type=F32)
    value = jnp.einsum("cp,cd->dp", normed, w_value, preferred_element_type=F32)
    return (jax.nn.sigmoid(opened) * value * mask).astype(BF)


def block(
    pair,
    single,
    token_mask,
    pair_gain,
    w_ab,
    w_out_gate,
    x_gain,
    w_tri_out,
    bias_gain,
    w_bias,
    single_gain,
    w_query,
    w_key,
    w_value_gate,
    w_mix,
):
    chans, rows, width = pair.shape
    nq = C // chans
    part = rows // nq
    spots = part * width
    r = lax.axis_index(ROW)
    q = lax.axis_index(CHAN)
    core = lax.axis_index("core")
    live = token_mask.astype(F32)

    local = w_query.shape[1]
    single_normed = layer_norm(single.astype(F32), single_gain[None, :], 1).astype(BF)
    own_keys = jnp.dot(single_normed, w_key, preferred_element_type=F32).astype(BF)
    own_values = jnp.dot(single_normed, w_value_gate[:, 0, :], preferred_element_type=F32).astype(BF)
    queries = jnp.dot(single_normed, w_query, preferred_element_type=F32).astype(BF)
    head_gate = jax.nn.sigmoid(
        jnp.dot(single_normed, w_value_gate[:, 1, :], preferred_element_type=F32)
    )
    gate_high = lax.reduce_precision(head_gate, 8, 7)
    gate_rest = (head_gate - gate_high).astype(BF)
    rest = jnp.concatenate(
        [filled(queries, gate_high.astype(BF)), filled(gate_rest)]
        + [w_mix[:, k : k + LANES] for k in range(0, D, LANES)]
    )
    kv = filled(own_keys, own_values)[None, None, None]
    kv = doubled(kv, "y", 1, 0)
    kv = doubled(kv, "x", 1, 1)
    kv = doubled(kv, "zl", 1, 2)
    kv = kv.reshape(-1, LANES)
    split = kv.shape[0]
    both = doubled(jnp.concatenate([kv, rest])[None], "zh", 0, 0)
    kv = both[:, :split].reshape(2, 2, 1, 2, 1, 2, 1, 1, rows, LANES)
    rest = both[:, split:]
    kv = doubled(kv, "y", 0, 2)
    kv = doubled(kv, "x", 0, 4)
    kv = doubled(kv, "zl", 0, 6)
    kv = doubled(kv, "core", 0, 7)
    kv = kv.reshape(nq, -1, LANES)
    rest = doubled(rest[:, None, None], "y", 0, 2)
    rest = doubled(rest, "y", 1, 1).reshape(nq, -1, LANES)

    sent = pair.reshape(chans, nq, spots).transpose(1, 0, 2)
    full = swap(sent, CHAN).reshape(C, spots).astype(F32)
    normed = layer_norm(full, pair_gain[:, None], 0).astype(BF)
    live_rows = lax.dynamic_slice_in_dim(live, r * rows + q * part, part, 0)
    mask = (live_rows[:, None] * live[None, :]).reshape(1, spots)
    left = edge(normed, w_ab[:, 0], w_ab[:, 1], mask).reshape(C, 2, spots // 2)
    right = edge(normed, w_ab[:, 2], w_ab[:, 3], mask).reshape(C, 2, spots // 2)
    edges = swap(jnp.concatenate([right, left], axis=2), OWN)
    right_here = edges[:, :, : spots // 2].reshape(C // nq, rows, width)
    right_there = lax.ppermute(right_here, "core", [(0, 1), (1, 0)])
    left_owned = edges[:, :, spots // 2 :].reshape(C * part, width)
    first = core == 0
    right_owned = jnp.stack(
        [
            jnp.where(first, right_here, right_there),
            jnp.where(first, right_there, right_here),
        ],
        axis=1,
    ).reshape(2 * C * part, width)
    owned = lax.dot_general(
        left_owned, right_owned, (((1,), (1,)), ((), ())), preferred_element_type=F32
    ).astype(BF)
    product = swap(owned.reshape(C, 2, spots // 2), OWN).reshape(C, spots)

    product_normed = layer_norm(product.astype(F32), x_gain[:, None], 0).astype(BF)
    out_gate = jax.nn.sigmoid(
        jnp.einsum("cp,cd->dp", normed, w_out_gate, preferred_element_type=F32)
    )
    update = jnp.einsum("cp,cd->dp", product_normed, w_tri_out, preferred_element_type=F32)
    renewed = (full + out_gate * update).astype(BF)
    bias_input = layer_norm(renewed.astype(F32), bias_gain[:, None], 0).astype(BF)
    by_head = w_bias.reshape(C, nq // 2, 2, -1).transpose(0, 2, 1, 3).reshape(w_bias.shape)
    bias = jnp.einsum("cp,ch->hp", bias_input, by_head, preferred_element_type=F32)

    heads = H // nq
    head_size = D // H
    at = q * part
    mine = lax.dynamic_slice_in_dim(rest, at, part, 1)
    gate_mine = mine[..., local : 2 * local].astype(F32) + lax.dynamic_slice_in_dim(
        rest, rows + at, part, 1
    )[..., :local].astype(F32)
    is_head = (jnp.arange(local)[None, :] // head_size == jnp.arange(heads)[:, None])[:, None]
    queries = jnp.where(is_head, mine[:, None, :, :local], 0).reshape(nq, heads * part, local)
    scores = jnp.einsum("qaf,qjf->qaj", queries, kv[..., :local], preferred_element_type=F32)
    scores = scores / jnp.sqrt(F32(head_size)) + bias.reshape(nq, heads * part, width)
    scores = jnp.where(live[None, None, :] > 0, scores, -jnp.inf)
    top = jnp.max(scores, axis=2, keepdims=True)
    raised = jnp.exp(scores - top)
    weights = (raised / jnp.sum(raised, axis=2, keepdims=True)).astype(BF)
    mixed = jnp.einsum(
        "qaj,qjf->qaf", weights, kv[..., local : 2 * local], preferred_element_type=F32
    )
    mixed = jnp.where(is_head, mixed.reshape(nq, heads, part, local), 0).sum(axis=1)
    heads_out = (mixed * gate_mine).astype(BF).transpose(1, 0, 2).reshape(part, D)
    mix = rest[:, 2 * rows :].reshape(nq, D // LANES, local, LANES).transpose(0, 2, 1, 3)
    summed = jnp.dot(heads_out, mix.reshape(D, D), preferred_element_type=F32).astype(BF)
    summed = summed.reshape(part, nq, local).transpose(1, 0, 2)
    summed = jnp.pad(summed, ((0, 0), (0, chans - part), (0, LANES - local)))
    sent = jnp.concatenate([renewed.reshape(nq, chans, spots), summed], axis=2)
    both = swap(sent, CHAN)
    pair_out = both[:, :, :spots].transpose(1, 0, 2).reshape(chans, rows, width)
    attended = both[:, :part, spots : spots + local].reshape(rows, local)
    return (pair_out, attended)


def solution(mesh):
    split = Mesh(mesh.devices.reshape(4, 4, 2, 4, 2), ROW + CHAN)
    return jax.shard_map(
        block,
        mesh=split,
        in_specs=(
            P(CHAN, ROW, None),
            P(ROW, None),
            P(),
            P(),
            P(),
            P(),
            P(),
            P(),
            P(),
            P(),
            P(),
            P(None, CHAN),
            P(None, CHAN),
            P(None, None, CHAN),
            P(CHAN, None),
        ),
        out_specs=(P(CHAN, ROW, None), P(ROW, CHAN)),
        check_vma=False,
    )
```

```python
import jax
import jax.numpy as jnp
from jax import lax
from jax.sharding import Mesh
from jax.sharding import PartitionSpec as P

D = 384
H = 16
C = 128
EPS = 1e-05
LANES = 128
ROW = ("x", "zl", "core")
CHAN = ("y", "zh")
OWN = ("x", "zl", "y", "zh")
BF = jnp.bfloat16
F32 = jnp.float32


def layer_norm(values, gain, axis):
    middle = jnp.mean(values, axis=axis, keepdims=True)
    centred = values - middle
    spread = jnp.mean(centred * centred, axis=axis, keepdims=True)
    return centred * lax.rsqrt(spread + EPS) * gain


def swap(shard, axes):
    return lax.all_to_all(shard, axes, 0, 0, tiled=True)


def doubled(block, axis, bit, dim):
    size = lax.axis_size(axis)
    there = lax.ppermute(block, axis, [(i, i ^ (1 << bit)) for i in range(size)])
    low = (lax.axis_index(axis) >> bit) & 1 == 0
    return jnp.concatenate([jnp.where(low, block, there), jnp.where(low, there, block)], axis=dim)


def rows_in_order(spread, part, nq):
    width = spread.shape[1] // part
    pieces = [spread[:, width * t : width * (t + 1)].reshape(-1, nq, width) for t in range(part)]
    return jnp.concatenate(pieces, axis=1)


def filled(*parts):
    wide = jnp.concatenate(parts, axis=-1)
    return jnp.pad(wide, [(0, 0)] * (wide.ndim - 1) + [(0, LANES - wide.shape[-1])])


def edge(normed, w_gate, w_value, mask):
    opened = jnp.einsum("cp,cd->dp", normed, w_gate, preferred_element_type=F32)
    value = jnp.einsum("cp,cd->dp", normed, w_value, preferred_element_type=F32)
    return (jax.nn.sigmoid(opened) * value * mask).astype(BF)


def block(
    pair,
    single,
    token_mask,
    pair_gain,
    w_ab,
    w_out_gate,
    x_gain,
    w_tri_out,
    bias_gain,
    w_bias,
    single_gain,
    w_query,
    w_key,
    w_value_gate,
    w_mix,
):
    chans, rows, width = pair.shape
    nq = C // chans
    part = rows // nq
    spots = part * width
    r = lax.axis_index(ROW)
    q = lax.axis_index(CHAN)
    core = lax.axis_index("core")
    live = token_mask.astype(F32)

    local = w_query.shape[1]
    single_normed = layer_norm(single.astype(F32), single_gain[None, :], 1).astype(BF)
    own_keys = jnp.dot(single_normed, w_key, preferred_element_type=F32).astype(BF)
    own_values = jnp.dot(single_normed, w_value_gate[:, 0, :], preferred_element_type=F32).astype(BF)
    queries = jnp.dot(single_normed, w_query, preferred_element_type=F32).astype(BF)
    head_gate = jax.nn.sigmoid(
        jnp.dot(single_normed, w_value_gate[:, 1, :], preferred_element_type=F32)
    )
    gate_high = lax.reduce_precision(head_gate, 8, 7)
    gate_rest = (head_gate - gate_high).astype(BF)
    rest = jnp.concatenate(
        [filled(queries, gate_high.astype(BF)), filled(gate_rest)]
        + [w_mix[:, k : k + LANES] for k in range(0, D, LANES)]
    )
    kv = filled(own_keys, own_values)[None, None, None]
    kv = doubled(kv, "y", 1, 0)
    kv = doubled(kv, "x", 1, 1)
    kv = doubled(kv, "zl", 1, 2)
    kv = kv.reshape(-1, LANES)
    split = kv.shape[0]
    both = doubled(jnp.concatenate([kv, rest])[None], "zh", 0, 0)
    kv = both[:, :split].reshape(2, 2, 1, 2, 1, 2, 1, 1, rows, LANES)
    rest = both[:, split:]
    kv = doubled(kv, "y", 0, 2)
    kv = doubled(kv, "x", 0, 4)
    kv = doubled(kv, "zl", 0, 6)
    kv = doubled(kv, "core", 0, 7)
    kv = kv.reshape(nq, -1, LANES)
    rest = doubled(rest[:, None, None], "y", 0, 2)
    rest = doubled(rest, "y", 1, 1).reshape(nq, -1, LANES)

    sent = jnp.concatenate([pair[:, nq * t : nq * (t + 1)] for t in range(part)], axis=2)
    sent = sent.transpose(1, 0, 2)
    full = swap(sent, CHAN).reshape(C, spots).astype(F32)
    normed = layer_norm(full, pair_gain[:, None], 0).astype(BF)
    live_rows = lax.dynamic_slice_in_dim(live, r * rows, rows, 0).reshape(part, nq)
    live_rows = lax.dynamic_index_in_dim(live_rows, q, 1, keepdims=False)
    mask = (live_rows[:, None] * live[None, :]).reshape(1, spots)
    half = spots // 2
    left = edge(normed, w_ab[:, 0], w_ab[:, 1], mask)
    right = edge(normed, w_ab[:, 2], w_ab[:, 3], mask)
    sent = [right[:, :half], left[:, :half], right[:, half:], left[:, half:]]
    sent = jnp.concatenate(sent, axis=1).reshape(C, 2, spots)

    edges = swap(sent, OWN)
    right_here = rows_in_order(edges[:, :, :half].reshape(C, spots), part, nq)
    right_there = lax.ppermute(right_here, "core", [(0, 1), (1, 0)])
    left_owned = edges[:, :, half:].reshape(C, spots)
    first = core == 0
    right_owned = jnp.stack(
        [
            jnp.where(first, right_here, right_there),
            jnp.where(first, right_there, right_here),
        ],
        axis=1,
    ).reshape(2 * C * part, width)
    owned = [
        lax.dot_general(
            left_owned[:, width * t : width * (t + 1)],
            right_owned,
            (((1,), (1,)), ((), ())),
            preferred_element_type=F32,
        ).astype(BF)
        for t in range(part)
    ]
    owned = jnp.concatenate(owned, axis=1).reshape(C, 2, half)
    product = swap(owned, OWN).reshape(C, spots)

    product_normed = layer_norm(product.astype(F32), x_gain[:, None], 0).astype(BF)
    out_gate = jax.nn.sigmoid(
        jnp.einsum("cp,cd->dp", normed, w_out_gate, preferred_element_type=F32)
    )
    update = jnp.einsum("cp,cd->dp", product_normed, w_tri_out, preferred_element_type=F32)
    renewed = (full + out_gate * update).astype(BF)
    bias_input = layer_norm(renewed.astype(F32), bias_gain[:, None], 0).astype(BF)
    by_head = w_bias.reshape(C, nq // 2, 2, -1).transpose(0, 2, 1, 3).reshape(w_bias.shape)
    bias = jnp.einsum("cp,ch->hp", bias_input, by_head, preferred_element_type=F32)

    heads = H // nq
    head_size = D // H
    mine = rest[:, : 2 * rows].reshape(nq, 2 * part, nq, LANES)
    mine = lax.dynamic_index_in_dim(mine, q, 2, keepdims=False)
    gate_mine = mine[:, :part, local : 2 * local].astype(F32) + mine[:, part:, :local].astype(F32)
    mine = mine[:, :part]
    is_head = (jnp.arange(local)[None, :] // head_size == jnp.arange(heads)[:, None])[:, None]
    queries = jnp.where(is_head, mine[:, None, :, :local], 0).reshape(nq, heads * part, local)
    scores = jnp.einsum("qaf,qjf->qaj", queries, kv[..., :local], preferred_element_type=F32)
    scores = scores / jnp.sqrt(F32(head_size)) + bias.reshape(nq, heads * part, width)
    scores = jnp.where(live[None, None, :] > 0, scores, -jnp.inf)
    top = jnp.max(scores, axis=2, keepdims=True)
    raised = jnp.exp(scores - top)
    weights = (raised / jnp.sum(raised, axis=2, keepdims=True)).astype(BF)
    mixed = jnp.einsum(
        "qaj,qjf->qaf", weights, kv[..., local : 2 * local], preferred_element_type=F32
    )
    mixed = jnp.where(is_head, mixed.reshape(nq, heads, part, local), 0).sum(axis=1)
    heads_out = (mixed * gate_mine).astype(BF).transpose(1, 0, 2).reshape(part, D)
    mix = rest[:, 2 * rows :].reshape(nq, D // LANES, local, LANES).transpose(0, 2, 1, 3)
    summed = jnp.dot(heads_out, mix.reshape(D, D), preferred_element_type=F32).astype(BF)
    summed = summed.reshape(part, nq, local).transpose(1, 0, 2)
    summed = jnp.pad(summed, ((0, 0), (0, chans - part), (0, LANES - local)))
    sent = jnp.concatenate([renewed.reshape(nq, chans, spots), summed], axis=2)
    both = swap(sent, CHAN)
    pair_out = both[:, :, :spots].transpose(1, 0, 2).reshape(chans * nq, spots)
    pair_out = rows_in_order(pair_out, part, nq)
    attended = both[:, :part, spots : spots + local].transpose(1, 0, 2).reshape(rows, local)
    return (pair_out, attended)


def solution(mesh):
    split = Mesh(mesh.devices.reshape(4, 4, 2, 4, 2), ROW + CHAN)
    return jax.shard_map(
        block,
        mesh=split,
        in_specs=(
            P(CHAN, ROW, None),
            P(ROW, None),
            P(),
            P(),
            P(),
            P(),
            P(),
            P(),
            P(),
            P(),
            P(),
            P(None, CHAN),
            P(None, CHAN),
            P(None, None, CHAN),
            P(CHAN, None),
        ),
        out_specs=(P(CHAN, ROW, None), P(ROW, CHAN)),
        check_vma=False,
    )
```

```python
import jax
import jax.numpy as jnp
from jax import lax
from jax.sharding import Mesh
from jax.sharding import PartitionSpec as P

D = 384
H = 16
C = 128
EPS = 1e-05
LANES = 128
ROW = ("x", "zl", "core")
CHAN = ("y", "zh")
SWAP = ("zh", "y")
OWN = ("x", "zl", "zh", "y")
BF = jnp.bfloat16
F32 = jnp.float32


def layer_norm(values, gain, axis):
    middle = jnp.mean(values, axis=axis, keepdims=True)
    centred = values - middle
    spread = jnp.mean(centred * centred, axis=axis, keepdims=True)
    return centred * lax.rsqrt(spread + EPS) * gain


def swap(shard, axes):
    return lax.all_to_all(shard, axes, 0, 0, tiled=True)


def doubled(block, axis, bit, dim):
    size = lax.axis_size(axis)
    there = lax.ppermute(block, axis, [(i, i ^ (1 << bit)) for i in range(size)])
    low = (lax.axis_index(axis) >> bit) & 1 == 0
    return jnp.concatenate([jnp.where(low, block, there), jnp.where(low, there, block)], axis=dim)


def rows_in_order(spread, part, nq):
    width = spread.shape[1] // part
    pieces = [spread[:, width * t : width * (t + 1)].reshape(-1, nq, width) for t in range(part)]
    return jnp.concatenate(pieces, axis=1)


def filled(*parts):
    wide = jnp.concatenate(parts, axis=-1)
    return jnp.pad(wide, [(0, 0)] * (wide.ndim - 1) + [(0, LANES - wide.shape[-1])])


def edge(normed, w_gate, w_value, mask):
    opened = jnp.einsum("cp,cd->dp", normed, w_gate, preferred_element_type=F32)
    value = jnp.einsum("cp,cd->dp", normed, w_value, preferred_element_type=F32)
    return (jax.nn.sigmoid(opened) * value * mask).astype(BF)


def block(
    pair,
    single,
    token_mask,
    pair_gain,
    w_ab,
    w_out_gate,
    x_gain,
    w_tri_out,
    bias_gain,
    w_bias,
    single_gain,
    w_query,
    w_key,
    w_value_gate,
    w_mix,
):
    chans, rows, width = pair.shape
    nq = C // chans
    part = rows // nq
    spots = part * width
    r = lax.axis_index(ROW)
    q = lax.axis_index(SWAP)
    core = lax.axis_index("core")
    live = token_mask.astype(F32)

    local = w_query.shape[1]
    single_normed = layer_norm(single.astype(F32), single_gain[None, :], 1).astype(BF)
    own_keys = jnp.dot(single_normed, w_key, preferred_element_type=F32).astype(BF)
    own_values = jnp.dot(single_normed, w_value_gate[:, 0, :], preferred_element_type=F32).astype(BF)
    queries = jnp.dot(single_normed, w_query, preferred_element_type=F32).astype(BF)
    head_gate = jax.nn.sigmoid(
        jnp.dot(single_normed, w_value_gate[:, 1, :], preferred_element_type=F32)
    )
    gate_high = lax.reduce_precision(head_gate, 8, 7)
    gate_rest = (head_gate - gate_high).astype(BF)
    rest = jnp.concatenate(
        [filled(queries, gate_high.astype(BF)), filled(gate_rest)]
        + [w_mix[:, k : k + LANES] for k in range(0, D, LANES)]
    )
    kv = filled(own_keys, own_values)[None, None, None]
    kv = doubled(kv, "y", 1, 0)
    kv = doubled(kv, "x", 1, 1)
    kv = doubled(kv, "zl", 1, 2)
    kv = kv.reshape(-1, LANES)
    split = kv.shape[0]
    both = doubled(jnp.concatenate([kv, rest])[None], "zh", 0, 0)
    kv = both[:, :split].reshape(2, 2, 1, 2, 1, 2, 1, 1, rows, LANES)
    rest = both[:, split:]
    kv = doubled(kv, "y", 0, 2)
    kv = doubled(kv, "x", 0, 4)
    kv = doubled(kv, "zl", 0, 6)
    kv = doubled(kv, "core", 0, 7)
    kv = kv.reshape(nq, -1, LANES)
    rest = doubled(rest[:, None, None], "y", 0, 2)
    rest = doubled(rest, "y", 1, 1).reshape(nq, -1, LANES)

    def by_place(values, axis):
        shape = values.shape
        values = values.reshape(shape[:axis] + (nq // 2, 2, -1) + shape[axis + 1 :])
        return values.swapaxes(axis, axis + 1).reshape(shape)

    pair_gain = by_place(pair_gain, 0)
    w_ab = by_place(w_ab, 0)
    bias_gain = by_place(bias_gain, 0)
    w_out_gate = by_place(by_place(w_out_gate, 0), 1)
    w_tri_out = by_place(w_tri_out, 1)
    w_bias = by_place(by_place(w_bias, 0), 1)

    sent = jnp.concatenate([pair[:, nq * t : nq * (t + 1)] for t in range(part)], axis=2)
    sent = sent.transpose(1, 0, 2)
    full = swap(sent, SWAP).reshape(C, spots).astype(F32)
    normed = layer_norm(full, pair_gain[:, None], 0).astype(BF)
    live_rows = lax.dynamic_slice_in_dim(live, r * rows, rows, 0).reshape(part, nq)
    live_rows = lax.dynamic_index_in_dim(live_rows, q, 1, keepdims=False)
    mask = (live_rows[:, None] * live[None, :]).reshape(1, spots)
    half = spots // 2
    left = edge(normed, w_ab[:, 0], w_ab[:, 1], mask)
    right = edge(normed, w_ab[:, 2], w_ab[:, 3], mask)
    sent = [right[:, :half], left[:, :half], right[:, half:], left[:, half:]]
    sent = jnp.concatenate(sent, axis=1).reshape(C, 2, spots)

    edges = swap(sent, OWN)
    right_here = rows_in_order(edges[:, :, :half].reshape(C, spots), part, nq)
    right_there = lax.ppermute(right_here, "core", [(0, 1), (1, 0)])
    left_owned = edges[:, :, half:].reshape(C, spots)
    first = core == 0
    right_owned = jnp.stack(
        [
            jnp.where(first, right_here, right_there),
            jnp.where(first, right_there, right_here),
        ],
        axis=1,
    ).reshape(2 * C * part, width)
    owned = [
        lax.dot_general(
            left_owned[:, width * t : width * (t + 1)],
            right_owned,
            (((1,), (1,)), ((), ())),
            preferred_element_type=F32,
        ).astype(BF)
        for t in range(part)
    ]
    owned = jnp.concatenate(owned, axis=1).reshape(C, 2, half)
    product = swap(owned, OWN).reshape(C, spots)

    product_normed = layer_norm(product.astype(F32), x_gain[:, None], 0).astype(BF)
    out_gate = jax.nn.sigmoid(
        jnp.einsum("cp,cd->dp", normed, w_out_gate, preferred_element_type=F32)
    )
    update = jnp.einsum("cp,cd->dp", product_normed, w_tri_out, preferred_element_type=F32)
    renewed = (full + out_gate * update).astype(BF)
    bias_input = layer_norm(renewed.astype(F32), bias_gain[:, None], 0).astype(BF)
    bias = jnp.einsum("cp,ch->hp", bias_input, w_bias, preferred_element_type=F32)

    heads = H // nq
    head_size = D // H
    mine = rest[:, : 2 * rows].reshape(nq, 2 * part, nq, LANES)
    mine = lax.dynamic_index_in_dim(mine, q, 2, keepdims=False)
    gate_mine = mine[:, :part, local : 2 * local].astype(F32) + mine[:, part:, :local].astype(F32)
    mine = mine[:, :part]
    is_head = (jnp.arange(local)[None, :] // head_size == jnp.arange(heads)[:, None])[:, None]
    queries = jnp.where(is_head, mine[:, None, :, :local], 0).reshape(nq, heads * part, local)
    scores = jnp.einsum("qaf,qjf->qaj", queries, kv[..., :local], preferred_element_type=F32)
    scores = scores / jnp.sqrt(F32(head_size)) + bias.reshape(nq, heads * part, width)
    scores = jnp.where(live[None, None, :] > 0, scores, -jnp.inf)
    top = jnp.max(scores, axis=2, keepdims=True)
    raised = jnp.exp(scores - top)
    weights = (raised / jnp.sum(raised, axis=2, keepdims=True)).astype(BF)
    mixed = jnp.einsum(
        "qaj,qjf->qaf", weights, kv[..., local : 2 * local], preferred_element_type=F32
    )
    mixed = jnp.where(is_head, mixed.reshape(nq, heads, part, local), 0).sum(axis=1)
    heads_out = (mixed * gate_mine).astype(BF).transpose(1, 0, 2).reshape(part, D)
    mix = rest[:, 2 * rows :].reshape(nq, D // LANES, local, LANES).transpose(0, 2, 1, 3)
    mix = by_place(mix.reshape(D, D), 1)
    summed = jnp.dot(heads_out, mix, preferred_element_type=F32).astype(BF)
    summed = summed.reshape(part, nq, local).transpose(1, 0, 2)
    summed = jnp.pad(summed, ((0, 0), (0, chans - part), (0, LANES - local)))
    sent = jnp.concatenate([renewed.reshape(nq, chans, spots), summed], axis=2)
    both = swap(sent, SWAP)
    pair_out = both[:, :, :spots].transpose(1, 0, 2).reshape(chans * nq, spots)
    pair_out = rows_in_order(pair_out, part, nq)
    attended = both[:, :part, spots : spots + local].transpose(1, 0, 2).reshape(rows, local)
    return (pair_out, attended)


def solution(mesh):
    split = Mesh(mesh.devices.reshape(4, 4, 2, 4, 2), ROW + CHAN)
    return jax.shard_map(
        block,
        mesh=split,
        in_specs=(
            P(CHAN, ROW, None),
            P(ROW, None),
            P(),
            P(),
            P(),
            P(),
            P(),
            P(),
            P(),
            P(),
            P(),
            P(None, CHAN),
            P(None, CHAN),
            P(None, None, CHAN),
            P(CHAN, None),
        ),
        out_specs=(P(CHAN, ROW, None), P(ROW, CHAN)),
        check_vma=False,
    )
```

```python
import jax
import jax.numpy as jnp
from jax import lax
from jax.sharding import Mesh
from jax.sharding import PartitionSpec as P

D = 384
H = 16
C = 128
EPS = 1e-05
LANES = 128
ROW = ("x", "zl", "core")
CHAN = ("y", "zh")
OWN = ("x", "zl", "y", "zh")
BF = jnp.bfloat16
F32 = jnp.float32


def layer_norm(values, gain, axis):
    middle = jnp.mean(values, axis=axis, keepdims=True)
    centred = values - middle
    spread = jnp.mean(centred * centred, axis=axis, keepdims=True)
    return centred * lax.rsqrt(spread + EPS) * gain


def swap(shard, axes):
    return lax.all_to_all(shard, axes, 0, 0, tiled=True)


def doubled(block, axis, bit, dim):
    size = lax.axis_size(axis)
    there = lax.ppermute(block, axis, [(i, i ^ (1 << bit)) for i in range(size)])
    low = (lax.axis_index(axis) >> bit) & 1 == 0
    return jnp.concatenate([jnp.where(low, block, there), jnp.where(low, there, block)], axis=dim)


def rows_in_order(spread, part, nq):
    width = spread.shape[1] // part
    pieces = [spread[:, width * t : width * (t + 1)].reshape(-1, nq, width) for t in range(part)]
    return jnp.concatenate(pieces, axis=1)


def filled(*parts):
    wide = jnp.concatenate(parts, axis=-1)
    return jnp.pad(wide, [(0, 0)] * (wide.ndim - 1) + [(0, LANES - wide.shape[-1])])


def edge(normed, w_gate, w_value, mask):
    opened = jnp.einsum("cp,cd->dp", normed, w_gate, preferred_element_type=F32)
    value = jnp.einsum("cp,cd->dp", normed, w_value, preferred_element_type=F32)
    return (jax.nn.sigmoid(opened) * value * mask).astype(BF)


def block(
    pair,
    single,
    token_mask,
    pair_gain,
    w_ab,
    w_out_gate,
    x_gain,
    w_tri_out,
    bias_gain,
    w_bias,
    single_gain,
    w_query,
    w_key,
    w_value_gate,
    w_mix,
):
    chans, rows, width = pair.shape
    nq = C // chans
    part = rows // nq
    spots = part * width
    r = lax.axis_index(ROW)
    q = lax.axis_index(CHAN)
    core = lax.axis_index("core")
    live = token_mask.astype(F32)

    local = w_query.shape[1]
    single_normed = layer_norm(single.astype(F32), single_gain[None, :], 1).astype(BF)
    own_keys = jnp.dot(single_normed, w_key, preferred_element_type=F32).astype(BF)
    own_values = jnp.dot(single_normed, w_value_gate[:, 0, :], preferred_element_type=F32).astype(BF)
    queries = jnp.dot(single_normed, w_query, preferred_element_type=F32).astype(BF)
    head_gate = jax.nn.sigmoid(
        jnp.dot(single_normed, w_value_gate[:, 1, :], preferred_element_type=F32)
    )
    gate_high = lax.reduce_precision(head_gate, 8, 7)
    gate_rest = (head_gate - gate_high).astype(BF)
    rest = jnp.concatenate(
        [filled(queries, gate_high.astype(BF)), filled(gate_rest)]
        + [w_mix[:, k : k + LANES] for k in range(0, D, LANES)]
    )
    kv = filled(own_keys, own_values)[None, None, None]
    kv = doubled(kv, "y", 1, 0)
    kv = doubled(kv, "x", 1, 1)
    kv = doubled(kv, "zl", 1, 2)
    kv = kv.reshape(-1, LANES)
    split = kv.shape[0]
    both = doubled(jnp.concatenate([kv, rest])[None], "zh", 0, 0)
    kv = both[:, :split].reshape(2, 2, 1, 2, 1, 2, 1, 1, rows, LANES)
    rest = both[:, split:]
    kv = doubled(kv, "y", 0, 2)
    kv = doubled(kv, "x", 0, 4)
    kv = doubled(kv, "zl", 0, 6)
    kv = doubled(kv, "core", 0, 7)
    kv = kv.reshape(nq, -1, LANES)
    rest = doubled(rest[:, None, None], "y", 0, 2)
    rest = doubled(rest, "y", 1, 1).reshape(nq, -1, LANES)

    sent = jnp.concatenate([pair[:, nq * t : nq * (t + 1)] for t in range(part)], axis=2)
    sent = sent.transpose(1, 0, 2)
    full = swap(sent, CHAN).reshape(C, spots).astype(F32)
    normed = layer_norm(full, pair_gain[:, None], 0).astype(BF)
    live_rows = lax.dynamic_slice_in_dim(live, r * rows, rows, 0).reshape(part, nq)
    live_rows = lax.dynamic_index_in_dim(live_rows, q, 1, keepdims=False)
    mask = (live_rows[:, None] * live[None, :]).reshape(1, spots)
    half = spots // 2
    left = edge(normed, w_ab[:, 0], w_ab[:, 1], mask)
    right = edge(normed, w_ab[:, 2], w_ab[:, 3], mask)
    sent = [right[:, :half], left[:, :half], right[:, half:], left[:, half:]]
    sent = jnp.concatenate(sent, axis=1).reshape(C, 2, spots)

    edges = swap(sent, OWN)
    right_here = rows_in_order(edges[:, :, :half].reshape(C, spots), part, nq)
    right_there = lax.ppermute(right_here, "core", [(0, 1), (1, 0)])
    left_owned = edges[:, :, half:].reshape(C, spots)
    left_owned = [left_owned[:, width * t : width * (t + 1)] for t in range(part)]
    left_owned = jnp.concatenate(left_owned, axis=0)
    first = core == 0
    right_owned = jnp.stack(
        [
            jnp.where(first, right_here, right_there),
            jnp.where(first, right_there, right_here),
        ],
        axis=1,
    ).reshape(2 * C * part, width)
    owned = lax.dot_general(
        left_owned, right_owned, (((1,), (1,)), ((), ())), preferred_element_type=F32
    ).astype(BF)
    owned = jnp.concatenate([owned[C * t : C * (t + 1)] for t in range(part)], axis=1)
    owned = owned.reshape(C, 2, half)
    product = swap(owned, OWN).reshape(C, spots)
    product = lax.optimization_barrier(product)

    product_normed = layer_norm(product.astype(F32), x_gain[:, None], 0).astype(BF)
    out_gate = jax.nn.sigmoid(
        jnp.einsum("cp,cd->dp", normed, w_out_gate, preferred_element_type=F32)
    )
    update = jnp.einsum("cp,cd->dp", product_normed, w_tri_out, preferred_element_type=F32)
    renewed = (full + out_gate * update).astype(BF)
    bias_input = layer_norm(renewed.astype(F32), bias_gain[:, None], 0).astype(BF)
    by_head = w_bias.reshape(C, nq // 2, 2, -1).transpose(0, 2, 1, 3).reshape(w_bias.shape)
    bias = jnp.einsum("cp,ch->hp", bias_input, by_head, preferred_element_type=F32)

    heads = H // nq
    head_size = D // H
    mine = rest[:, : 2 * rows].reshape(nq, 2 * part, nq, LANES)
    mine = lax.dynamic_index_in_dim(mine, q, 2, keepdims=False)
    gate_mine = mine[:, :part, local : 2 * local].astype(F32) + mine[:, part:, :local].astype(F32)
    mine = mine[:, :part]
    is_head = (jnp.arange(local)[None, :] // head_size == jnp.arange(heads)[:, None])[:, None]
    queries = jnp.where(is_head, mine[:, None, :, :local], 0).reshape(nq, heads * part, local)
    scores = jnp.einsum("qaf,qjf->qaj", queries, kv[..., :local], preferred_element_type=F32)
    scores = scores / jnp.sqrt(F32(head_size)) + bias.reshape(nq, heads * part, width)
    scores = jnp.where(live[None, None, :] > 0, scores, -jnp.inf)
    top = jnp.max(scores, axis=2, keepdims=True)
    raised = jnp.exp(scores - top)
    weights = (raised / jnp.sum(raised, axis=2, keepdims=True)).astype(BF)
    mixed = jnp.einsum(
        "qaj,qjf->qaf", weights, kv[..., local : 2 * local], preferred_element_type=F32
    )
    mixed = jnp.where(is_head, mixed.reshape(nq, heads, part, local), 0).sum(axis=1)
    heads_out = (mixed * gate_mine).astype(BF).transpose(1, 0, 2).reshape(part, D)
    mix = rest[:, 2 * rows :].reshape(nq, D // LANES, local, LANES).transpose(0, 2, 1, 3)
    summed = jnp.dot(heads_out, mix.reshape(D, D), preferred_element_type=F32).astype(BF)
    summed = summed.reshape(part, nq, local).transpose(1, 0, 2)
    summed = jnp.pad(summed, ((0, 0), (0, chans - part), (0, LANES - local)))
    sent = jnp.concatenate([renewed.reshape(nq, chans, spots), summed], axis=2)
    both = swap(sent, CHAN)
    pair_out = both[:, :, :spots].transpose(1, 0, 2).reshape(chans * nq, spots)
    pair_out = rows_in_order(pair_out, part, nq)
    attended = both[:, :part, spots : spots + local].transpose(1, 0, 2).reshape(rows, local)
    return (pair_out, attended)


def solution(mesh):
    split = Mesh(mesh.devices.reshape(4, 4, 2, 4, 2), ROW + CHAN)
    return jax.shard_map(
        block,
        mesh=split,
        in_specs=(
            P(CHAN, ROW, None),
            P(ROW, None),
            P(),
            P(),
            P(),
            P(),
            P(),
            P(),
            P(),
            P(),
            P(),
            P(None, CHAN),
            P(None, CHAN),
            P(None, None, CHAN),
            P(CHAN, None),
        ),
        out_specs=(P(CHAN, ROW, None), P(ROW, CHAN)),
        check_vma=False,
    )
```
